32 devices in a mesh: dp: 8 (over y, x, core), tensor: 4 (over z).
Axes of the slice: x: 2, y: 2, z: 4, core: 2. Of those that a mesh axis runs over, the one named last changes fastest.
Arguments:
- hidden_in: bfloat16 [8, 128, 16384], P('dp'), may hold values from -6 to 6
- value_weight: bfloat16 [16384, 256], P(None, 'tensor'), may hold values from -0.046875 to 0.046875
- queries: bfloat16 [8, 128, 4096], P('dp', None, 'tensor'), may hold values from -4 to 4
- key_rows: bfloat16 [8, 128, 256], P('dp', None, 'tensor'), may hold values from -4 to 4
- attention_out: bfloat16 [8, 128, 4096], P('dp', None, 'tensor'), may hold values from -4 to 4
- output_grad: bfloat16 [8, 128, 4096], P('dp', None, 'tensor'), may hold values from -6 to 6
- log_normalizer: float32 [8, 128, 32], P('dp', None, 'tensor'), may hold values from 1 to 5
- document_ids: int32 [8, 128], P('dp'), may hold values from 0 to 3, never falling along the last dimension, each value on 1 to 64 neighbouring positions
Outputs:
- query_grad: bfloat16 [8, 128, 4096], P('dp', None, 'tensor')
- key_grad: bfloat16 [8, 128, 256], P('dp', None, 'tensor')
- input_grad: bfloat16 [8, 128, 16384], P('dp', 'tensor')
- value_weight_grad: float32 [16384, 256], P('dp', 'tensor')
The draws below stay inside these ranges and needn't reach their ends.
Inputs may be any that keep to these rules, and one draw needn't show every extreme that they name: `document_ids`: within one group the ids never fall; all 4 documents occur, each of 1 to 64 tokens.
All inputs are finite; a program needn't handle non-finite values.
Results may differ from the reference program's by a relative error of at most 0.014.
Values may be sent and summed in bfloat16 or wider, within the bound.
A program may use at most 64 MiB of HBM per device.

```python
import math
from functools import partial
import jax
import jax.numpy as jnp
import numpy as np
from jax import lax

D = 16384
HD = 128
GROUP = 16
TOK_DEV = 128
DOCS = 4
QHEADS = 32
KVH = 2
GROUPS = 8


def raised(values, own_key, source, target, shards_of, factor):
    owner, partner = [(jnp.arange(values.shape[dim]) // (values.shape[dim] // shards_of)).reshape([-1 if axis == dim else 1 for axis in range(values.ndim)]) for dim in (source, target)]
    chosen = jax.random.permutation(own_key, shards_of)[partner]
    strong = (owner == chosen) | (owner == (partner + shards_of // 2) % shards_of)
    return jnp.where(strong, factor * values, values)


def block_scale(stream_key, shape, pieces, smallest, high):
    level = 1.0
    for dim, parts in pieces:
        draws = jax.random.uniform(jax.random.fold_in(jax.random.fold_in(stream_key, 6), dim), (parts,), jnp.float32, smallest / len(pieces), high / len(pieces))
        level = level * jnp.repeat(jnp.exp(draws), shape[dim] // parts).reshape((-1,) + (1,) * (len(shape) - 1 - dim))
    return level


def profile(count, total, reach, lean):
    loads = [(1 << 20) // math.isqrt(grade ** lean) + 1 for grade in range(2, count + 1)]
    spare, counts = total - reach - (count - 1), [1] * (count - 1)
    while spare > 0:
        candidates = [i for i in range(count - 1) if counts[i] < reach]
        whole, budget = sum([loads[i] for i in candidates]), spare
        for i in candidates:
            addition = min(reach - counts[i], max(1, budget * loads[i] // whole), spare)
            counts[i] = counts[i] + addition
            spare = spare - addition
    return np.array([reach] + counts)


def uneven_parts(stream_key, amount, total, limit, skew):
    if amount == 2:
        one = jax.random.randint(stream_key, (), max(1, total - limit), min(limit, total - 1) + 1)
        return jnp.stack([one, total - one])
    sizes = jnp.asarray(profile(amount, total, limit, skew), jnp.int32)
    twos = (amount - 1) // 2
    source_of, sink = sizes[1:1 + 2 * twos:2], sizes[2:2 + 2 * twos:2]
    slack = jnp.minimum(source_of - 1, limit - sink)
    moved = jax.random.randint(jax.random.fold_in(stream_key, 1), (twos,), 0, 1 << 20) % (slack + 1)
    sizes = sizes.at[1:1 + 2 * twos:2].set(source_of - moved).at[2:2 + 2 * twos:2].set(sink + moved)
    return sizes[jax.random.permutation(jax.random.fold_in(stream_key, 2), amount)]


def gaussian(rng, extent, scale, reach, split=(), held_as=jnp.bfloat16):
    result = scale * jax.random.normal(rng, extent, jnp.float32)
    if split:
        result = result * block_scale(rng, extent, split, -0.22, 0.18)
    return jnp.clip(result, -reach, reach).astype(held_as)


def heavy_noise(key, dims, deviation, limit, split, heavy, kind=jnp.bfloat16):
    values = deviation * jax.random.normal(key, dims, jnp.float32)
    if split:
        values = values * block_scale(key, dims, split, -0.22, 0.18)
    return jnp.clip(raised(values, jax.random.fold_in(key, 3), *heavy), -limit, limit).astype(kind)


def setup_inputs(seed: int = 0) -> dict:
    keys = jax.random.split(jax.random.key(seed), 9)
    hidden_in = heavy_noise(keys[0], (GROUPS, TOK_DEV, D), 1.0, 6.0, ((0, 8),), (0, 2, 8, 2.0))
    value_weight = gaussian(keys[1], (D, KVH * HD), D ** -0.5, 0.046875, ((1, 4),))
    queries = gaussian(keys[2], (GROUPS, TOK_DEV, QHEADS * HD), 1.0, 4.0, ((0, 8), (2, 4)))
    key_rows = gaussian(keys[3], (GROUPS, TOK_DEV, KVH * HD), 1.0, 4.0, ((0, 8), (2, 4)))
    attention_out = gaussian(keys[4], (GROUPS, TOK_DEV, QHEADS * HD), 0.5, 4.0, ((0, 8), (2, 4)))
    output_grad = heavy_noise(keys[5], (GROUPS, TOK_DEV, QHEADS * HD), 1.0, 6.0, ((0, 8), (2, 4)), (2, 1, 4, 2.0))
    log_normalizer = jnp.clip(1.0 + 4.0 * jax.random.uniform(keys[6], (GROUPS, TOK_DEV, QHEADS), jnp.float32) ** block_scale(keys[6], (GROUPS, TOK_DEV, QHEADS), ((0, 8), (2, 4)), -0.2, 0.2), 1.0, 5.0)
    document_ids = jax.vmap(lambda own: jnp.searchsorted(jnp.cumsum(uneven_parts(own, DOCS, TOK_DEV, TOK_DEV // 2, 1)), jnp.arange(TOK_DEV), side="right"))(jax.random.split(keys[7], GROUPS)).reshape((GROUPS, TOK_DEV)).astype(jnp.int32)
    return {"hidden_in": hidden_in, "value_weight": value_weight, "queries": queries, "key_rows": key_rows, "attention_out": attention_out, "output_grad": output_grad, "log_normalizer": log_normalizer, "document_ids": document_ids}


def rounded(array):
    return lax.optimization_barrier(array.astype(jnp.bfloat16)).astype(jnp.float32)

def group_backward(value_weight, operands):
    hidden_in, queries, key_rows, attention_out, output_grad, log_normalizer, document_ids = operands
    tokens = hidden_in.shape[0]
    score_scale = 1.0 / math.sqrt(HD)
    values = jnp.dot(hidden_in, value_weight, preferred_element_type=jnp.float32).astype(jnp.bfloat16)
    query_heads = queries.astype(jnp.float32).reshape(tokens, KVH, GROUP, HD)
    key_heads = key_rows.astype(jnp.float32).reshape(tokens, KVH, HD)
    value_heads = values.astype(jnp.float32).reshape(tokens, KVH, HD)
    out_heads = attention_out.astype(jnp.float32).reshape(tokens, KVH, GROUP, HD)
    grad_heads = output_grad.astype(jnp.float32).reshape(tokens, KVH, GROUP, HD)
    normalizers = jnp.transpose(log_normalizer.reshape(tokens, KVH, GROUP), (1, 2, 0))[..., None]
    position = jnp.arange(tokens, dtype=jnp.int32)
    allowed = (position[None, :] <= position[:, None]) & (document_ids[:, None] == document_ids[None, :])
    scores = jnp.einsum('tcgd,scd->cgts', query_heads, key_heads) * score_scale
    probabilities = jnp.where(allowed, jnp.exp(scores - normalizers), 0.0)
    probs_low = rounded(probabilities)
    value_sum = jnp.einsum('cgts,tcgd->scd', probs_low, grad_heads)
    row_dots = jnp.einsum('tcgd,tcgd->cgt', grad_heads, out_heads)
    prob_grad = jnp.einsum('tcgd,scd->cgts', grad_heads, value_heads)
    score_grad = rounded(probabilities * (prob_grad - row_dots[..., None]) * score_scale)
    query_grad = jnp.einsum('cgts,scd->tcgd', score_grad, key_heads).astype(jnp.bfloat16)
    key_grad = jnp.einsum('cgts,tcgd->scd', score_grad, query_heads).astype(jnp.bfloat16)
    value_grad = value_sum.astype(jnp.bfloat16).reshape(tokens, KVH * HD)
    block_width = HD // 2

    def add_block(summed, block_index):
        offset = block_index * block_width
        row_block = lax.dynamic_slice_in_dim(value_grad, offset, block_width, 1)
        col_block = lax.dynamic_slice_in_dim(value_weight, offset, block_width, 1)
        product = lax.dot_general(row_block, col_block, (((1,), (1,)), ((), ())), preferred_element_type=jnp.float32)
        return (summed + rounded(product), None)
    start_sum = jnp.zeros((tokens, value_weight.shape[0]), jnp.float32)
    input_sum, unused = lax.scan(add_block, start_sum, jnp.arange(2 * KVH, dtype=jnp.int32))
    return (query_grad.reshape(tokens, KVH * GROUP * HD), key_grad.reshape(tokens, KVH * HD), input_sum.astype(jnp.bfloat16), value_grad)

def reference(hidden_in, value_weight, queries, key_rows, attention_out, output_grad, log_normalizer, document_ids):
    results = lax.map(partial(group_backward, value_weight), (hidden_in, queries, key_rows, attention_out, output_grad, log_normalizer, document_ids))
    query_grad, key_grad, input_grad, value_grad = results
    flat_inputs = hidden_in.reshape(-1, hidden_in.shape[2])
    flat_grads = value_grad.reshape(-1, value_grad.shape[2])
    value_weight_grad = lax.dot_general(flat_inputs, flat_grads, (((0,), (0,)), ((), ())), preferred_element_type=jnp.float32)
    return (query_grad, key_grad, input_grad, value_weight_grad)
```

```python
import functools
import math

import jax
import jax.numpy as jnp
from jax import lax
from jax.experimental import pallas as pl
from jax.experimental.pallas import tpu as pltpu
from jax.sharding import PartitionSpec as P

MESH = pl.DeviceIdType.MESH
F32 = jnp.float32
BF16 = jnp.bfloat16
NT = (((1,), (1,)), ((), ()))


def fused(
    groups,
    ranks,
    hidden_hbm,
    weight_hbm,
    queries_ref,
    key_ref,
    out_ref,
    grad_ref,
    norm_ref,
    doc_ref,
    qg_ref,
    kg_ref,
    ig_ref,
    wg_ref,
    hidden,
    weight,
    piece,
    keys_t,
    values_t,
    probs,
    part,
    got_part,
    grads_t,
    out_buf,
    core_send,
    core_got,
    chip_send,
    chip_got,
    load_sem,
    pair_send,
    pair_recv,
    wa_send,
    wa_recv,
    wb_send,
    wb_recv,
    vg_send,
    vg_recv,
    dc_send,
    dc_recv,
    dx_send,
    dx_recv,
    o_send,
    o_recv,
):
    d = lax.axis_index("dp")
    t = lax.axis_index("tensor")
    member = t % 2
    pair = t + 1 - 2 * member
    core = d % 2
    chip = d // 2
    other_core = d + 1 - 2 * core
    chips = groups // 2
    tokens, width = hidden.shape
    half = weight.shape[0]
    heads = norm_ref.shape[0]
    hd = 2 * half
    scale = 1.0 / math.sqrt(hd)
    span = width // ranks
    sub = span // groups
    rows = tokens // ranks
    wg_cols = width // groups

    def ds(index, size):
        return pl.ds(pl.multiple_of(index * size, size), size)

    def remote(src, dst, send, recv, **device):
        return pltpu.make_async_remote_copy(
            src_ref=src, dst_ref=dst, send_sem=send, recv_sem=recv,
            device_id=device, device_id_type=MESH,
        )

    started = []

    def send(src, dst, ssem, rsem, **device):
        copy = remote(src, dst, ssem, rsem, **device)
        copy.start()
        started.append(copy)

    load_w = pltpu.make_async_copy(weight_hbm, weight, load_sem.at[0])
    load_h = pltpu.make_async_copy(hidden_hbm, hidden, load_sem.at[1])
    load_p = pltpu.make_async_copy(
        weight_hbm.at[:, ds(t, span)], piece.at[ds(t, half), :], load_sem.at[2]
    )
    load_p.start()
    load_h.start()
    load_w.start()
    load_k = pltpu.make_async_copy(key_ref, keys_t.at[member], load_sem.at[3])
    load_k.start()

    barrier = pltpu.get_barrier_semaphore()
    for r in range(1, ranks):
        pl.semaphore_signal(barrier, inc=1, device_id={"tensor": (t + r) % ranks}, device_id_type=MESH)
    for i in range(1, groups):
        pl.semaphore_signal(barrier, inc=1, device_id={"dp": (d + i) % groups}, device_id_type=MESH)
    pl.semaphore_wait(barrier, ranks + groups - 2)

    send(key_ref, keys_t.at[member], pair_send.at[0], pair_recv.at[0], tensor=pair)
    for r in range(1, ranks):
        to = (t + r) % ranks
        send(
            weight_hbm.at[:, ds(to * groups + d, sub)],
            piece.at[ds(t, half), ds(d, sub)],
            wa_send.at[to], wa_recv.at[t], tensor=to,
        )

    lane = lax.broadcasted_iota(jnp.int32, (tokens, hd), 1)
    dots = jnp.zeros((tokens, hd), F32)
    for j in range(heads):
        cols = slice(j * hd, (j + 1) * hd)
        product = grad_ref[:, cols].astype(F32) * out_ref[:, cols].astype(F32)
        dots = jnp.where(lane == j, jnp.sum(product, axis=1, keepdims=True), dots)
    dots = dots.T
    doc_row = jnp.broadcast_to(doc_ref[...].astype(F32), (tokens, tokens))
    doc_col = doc_row.T
    s_index = lax.broadcasted_iota(jnp.int32, (tokens, tokens), 0)
    t_index = lax.broadcasted_iota(jnp.int32, (tokens, tokens), 1)
    allowed = (s_index <= t_index) & (doc_row == doc_col)

    load_k.wait()
    remote(key_ref, keys_t.at[1 - member], pair_send.at[0], pair_recv.at[0], tensor=pair).wait_recv()
    keys = keys_t[...].reshape(hd, tokens).astype(F32).T.astype(BF16)
    total = jnp.zeros((tokens, hd), F32)
    for j in range(heads):
        cols = slice(j * hd, (j + 1) * hd)
        scores = lax.dot_general(keys, queries_ref[:, cols], NT, preferred_element_type=F32) * scale
        prob = jnp.where(allowed, jnp.exp(scores - norm_ref[j : j + 1, :]), 0.0)
        probs[j] = prob
        total += jnp.dot(prob.astype(BF16), grad_ref[:, cols], preferred_element_type=F32)
    part[0] = total.T
    send(
        part.at[0, ds(1 - member, half), :], got_part.at[0],
        pair_send.at[1], pair_recv.at[1], tensor=pair,
    )

    for r in range(1, ranks):
        source = (t + r) % ranks
        block = piece.at[ds(source, half), ds(d, sub)]
        remote(block, block, wa_send.at[source], wa_recv.at[source], tensor=source).wait_recv()
        for i in range(1, groups):
            to = (d + i) % groups
            send(block, block, wb_send.at[source, to], wb_recv.at[source, d], dp=to)

    load_w.wait()
    load_h.wait()
    chunk = wg_cols
    value = jnp.zeros((half, tokens), F32)
    for c in range(width // chunk):
        cols = slice(c * chunk, (c + 1) * chunk)
        value += lax.dot_general(weight[:, cols], hidden[:, cols], NT, preferred_element_type=F32)
    values_t[member] = value.astype(BF16)
    send(values_t.at[member], values_t.at[member], pair_send.at[2], pair_recv.at[2], tensor=pair)

    remote(got_part.at[0], got_part.at[0], pair_send.at[1], pair_recv.at[1], tensor=pair).wait_recv()
    grad_own = (part[0, ds(member, half), :] + got_part[0]).astype(BF16)
    grads_t[ds(t, half), :] = grad_own
    for r in range(1, ranks):
        to = (t + r) % ranks
        block = grads_t.at[ds(t, half), :]
        send(block, block, vg_send.at[to], vg_recv.at[t], tensor=to)

    def partial_wg(owner):
        return jnp.dot(grad_own, hidden[:, ds(owner, wg_cols)], preferred_element_type=F32)

    for i in range(chips):
        c = (chip + 1 + i) % chips
        core_send[i] = partial_wg(c * 2 + 1 - core).astype(BF16)
        send(core_send.at[i], core_got.at[i], dc_send.at[i], dc_recv.at[i], dp=other_core)

    for r in range(1, ranks):
        source = (t + r) % ranks
        block = grads_t.at[ds(source, half), :]
        remote(block, block, vg_send.at[source], vg_recv.at[source], tensor=source).wait_recv()
    grads = grads_t[...].astype(F32).T.astype(BF16)
    load_p.wait()

    def input_chunk(i):
        g = (d + groups - i) % groups
        if i:
            for r in range(1, ranks):
                source = (t + r) % ranks
                block = piece.at[ds(source, half), ds(g, sub)]
                remote(block, block, wb_send.at[source, g], wb_recv.at[source, g], dp=g).wait_recv()
        out_buf[i] = jnp.dot(grads, piece[:, ds(g, sub)], preferred_element_type=F32).astype(BF16)
        place = ds(t * groups + g, sub)
        for r in range(1, ranks):
            to = (t + r) % ranks
            send(
                out_buf.at[i, ds(to, rows), :], ig_ref.at[:, place],
                o_send.at[to, g], o_recv.at[t, g], tensor=to,
            )
        ig_ref[:, place] = out_buf[i, ds(t, rows), :]

    input_chunk(0)

    for i in range(chips):
        remote(core_send.at[i], core_got.at[i], dc_send.at[i], dc_recv.at[i], dp=other_core).wait_recv()
        if i < chips - 1:
            c = (chip + 1 + i) % chips
            chip_send[i] = (partial_wg(c * 2 + core) + core_got[i].astype(F32)).astype(BF16)
            send(chip_send.at[i], chip_got.at[i], dx_send.at[i], dx_recv.at[i], dp=c * 2 + core)
    wg_ref[...] = partial_wg(d) + core_got[chips - 1].astype(F32)

    input_chunk(1)
    input_chunk(2)

    remote(values_t.at[1 - member], values_t.at[1 - member], pair_send.at[2], pair_recv.at[2], tensor=pair).wait_recv()
    values = values_t[...].reshape(hd, tokens).astype(F32).T.astype(BF16)
    total = jnp.zeros((tokens, hd), F32)
    for j in range(heads):
        cols = slice(j * hd, (j + 1) * hd)
        prob_grad = lax.dot_general(values, grad_ref[:, cols], NT, preferred_element_type=F32)
        score_grad = probs[j] * (prob_grad - dots[j : j + 1, :]) * scale
        total += jnp.dot(score_grad.astype(BF16), queries_ref[:, cols], preferred_element_type=F32)
        qg_ref[:, cols] = jnp.dot(
            score_grad.T.astype(BF16), keys, preferred_element_type=F32
        ).astype(BF16)
    part[1] = total.T
    send(
        part.at[1, ds(1 - member, half), :], got_part.at[1],
        pair_send.at[3], pair_recv.at[3], tensor=pair,
    )

    for i in range(3, groups):
        input_chunk(i)

    remote(got_part.at[1], got_part.at[1], pair_send.at[3], pair_recv.at[3], tensor=pair).wait_recv()
    kg_ref[...] = (part[1, ds(member, half), :] + got_part[1]).astype(BF16)

    for i in range(chips - 1):
        c = (chip + chips - 1 - i) % chips
        remote(chip_send.at[i], chip_got.at[i], dx_send.at[i], dx_recv.at[i], dp=c * 2 + core).wait_recv()
        wg_ref[...] += chip_got[i].astype(F32)

    for r in range(1, ranks):
        source = (t + r) % ranks
        for i in range(groups):
            g = (d + groups - i) % groups
            place = ig_ref.at[:, ds(source * groups + g, sub)]
            remote(
                out_buf.at[0, ds(source, rows), :], place,
                o_send.at[source, g], o_recv.at[source, g], tensor=source,
            ).wait_recv()
    for copy in started:
        copy.wait_send()


def fused_per_device(groups, ranks, hidden_in, value_weight, queries, key_rows, attention_out,
                     output_grad, log_normalizer, document_ids):
    _, tokens, width = hidden_in.shape
    half = value_weight.shape[1]
    hd = 2 * half
    heads = log_normalizer.shape[2]
    span = width // ranks
    sub = span // groups
    chips = groups // 2
    wg_cols = width // groups
    vmem = pl.BlockSpec(memory_space=pltpu.VMEM)
    hbm = pl.BlockSpec(memory_space=pl.ANY)
    sem = pltpu.SemaphoreType.DMA
    query_grad, key_grad, input_grad, weight_grad = pl.pallas_call(
        functools.partial(fused, groups, ranks),
        out_shape=(
            jax.ShapeDtypeStruct((tokens, heads * hd), BF16),
            jax.ShapeDtypeStruct((half, tokens), BF16),
            jax.ShapeDtypeStruct((tokens // ranks, width), BF16),
            jax.ShapeDtypeStruct((half, wg_cols), F32),
        ),
        in_specs=[hbm, hbm] + [vmem] * 6,
        out_specs=(vmem,) * 4,
        scratch_shapes=[
            pltpu.VMEM((tokens, width), BF16),
            pltpu.VMEM((half, width), BF16),
            pltpu.VMEM((ranks * half, span), BF16),
            pltpu.VMEM((2, half, tokens), BF16),
            pltpu.VMEM((2, half, tokens), BF16),
            pltpu.VMEM((heads, tokens, tokens), F32),
            pltpu.VMEM((2, hd, tokens), F32),
            pltpu.VMEM((2, half, tokens), F32),
            pltpu.VMEM((ranks * half, tokens), BF16),
            pltpu.VMEM((groups, tokens, sub), BF16),
            pltpu.VMEM((chips, half, wg_cols), BF16),
            pltpu.VMEM((chips, half, wg_cols), BF16),
            pltpu.VMEM((chips - 1, half, wg_cols), BF16),
            pltpu.VMEM((chips - 1, half, wg_cols), BF16),
            sem((4,)),
            sem((4,)),
            sem((4,)),
            sem((ranks,)),
            sem((ranks,)),
            sem((ranks, groups)),
            sem((ranks, groups)),
            sem((ranks,)),
            sem((ranks,)),
            sem((chips,)),
            sem((chips,)),
            sem((chips,)),
            sem((chips,)),
            sem((ranks, groups)),
            sem((ranks, groups)),
        ],
        compiler_params=pltpu.CompilerParams(
            collective_id=0, has_side_effects=True, vmem_limit_bytes=40 * 1024 * 1024
        ),
    )(
        hidden_in[0],
        value_weight.T,
        queries[0],
        key_rows[0].T,
        attention_out[0],
        output_grad[0],
        log_normalizer[0].T,
        document_ids,
    )
    return query_grad[None], key_grad.T[None], input_grad[None], weight_grad.T


def partner(value, axis, distance):
    mask = 2**distance
    pairs = [(source, source ^ mask) for source in range(lax.axis_size(axis))]
    return lax.ppermute(value, axis, pairs)


def per_device(
    hidden_in,
    value_weight,
    queries,
    key_rows,
    attention_out,
    output_grad,
    log_normalizer,
    document_ids,
):
    tokens = hidden_in.shape[1]
    head_count = log_normalizer.shape[2]
    half_width = key_rows.shape[2]
    head_width = 2 * half_width
    score_scale = 1.0 / math.sqrt(head_width)
    inputs_local = hidden_in[0]
    value_half = jnp.dot(inputs_local, value_weight, preferred_element_type=jnp.float32).astype(
        jnp.bfloat16
    )
    key_half = key_rows[0]
    other_key, other_value = partner((key_half, value_half), "tensor", 0)
    pair_member = lax.axis_index("tensor") % 2
    lower_member = pair_member == 0
    keys_full = jnp.where(
        lower_member,
        jnp.concatenate([key_half, other_key], 1),
        jnp.concatenate([other_key, key_half], 1),
    )
    values_full = jnp.where(
        lower_member,
        jnp.concatenate([value_half, other_value], 1),
        jnp.concatenate([other_value, value_half], 1),
    )
    query_heads = queries[0].reshape(tokens, head_count, head_width)
    grad_heads = output_grad[0].reshape(tokens, head_count, head_width)
    out_heads = attention_out[0].reshape(tokens, head_count, head_width)
    position = jnp.arange(tokens, dtype=jnp.int32)
    documents = document_ids[0]
    allowed = (position[None, :] <= position[:, None]) & (documents[:, None] == documents[None, :])
    scores = (
        jnp.einsum("thd,sd->hts", query_heads, keys_full, preferred_element_type=jnp.float32)
        * score_scale
    )
    normalizers = jnp.transpose(log_normalizer[0])[:, :, None]
    probabilities = jnp.where(allowed[None], jnp.exp(scores - normalizers), 0.0)
    probs_low = probabilities.astype(jnp.bfloat16)
    value_part = jnp.einsum(
        "hts,thd->sd", probs_low, grad_heads, preferred_element_type=jnp.float32
    )
    row_dots = jnp.einsum("thd,thd->ht", grad_heads, out_heads, preferred_element_type=jnp.float32)
    prob_grad = jnp.einsum(
        "thd,sd->hts", grad_heads, values_full, preferred_element_type=jnp.float32
    )
    score_grad = (probabilities * (prob_grad - row_dots[:, :, None]) * score_scale).astype(
        jnp.bfloat16
    )
    query_grad = jnp.einsum(
        "hts,sd->thd", score_grad, keys_full, preferred_element_type=jnp.float32
    )
    query_grad = query_grad.astype(jnp.bfloat16).reshape(1, tokens, head_count * head_width)
    key_part = jnp.einsum(
        "hts,thd->sd", score_grad, query_heads, preferred_element_type=jnp.float32
    )
    own_offset = pair_member * half_width
    other_offset = (1 - pair_member) * half_width
    send_key = lax.dynamic_slice_in_dim(key_part, other_offset, half_width, 1)
    send_value = lax.dynamic_slice_in_dim(value_part, other_offset, half_width, 1)
    got_key, got_value = partner((send_key, send_value), "tensor", 0)
    key_sum = lax.dynamic_slice_in_dim(key_part, own_offset, half_width, 1) + got_key
    value_sum = lax.dynamic_slice_in_dim(value_part, own_offset, half_width, 1) + got_value
    key_grad = key_sum.astype(jnp.bfloat16).reshape(1, tokens, half_width)
    value_grad = value_sum.astype(jnp.bfloat16)
    input_sum = lax.psum_scatter(
        lax.dot_general(
            value_grad, value_weight, (((1,), (1,)), ((), ())), preferred_element_type=jnp.float32
        ).astype(jnp.bfloat16),
        "tensor",
        scatter_dimension=0,
        tiled=True,
    ).astype(jnp.float32)
    weight_grad = lax.psum_scatter(
        lax.dot_general(
            inputs_local, value_grad, (((0,), (0,)), ((), ())), preferred_element_type=jnp.float32
        ),
        "dp",
        scatter_dimension=0,
        tiled=True,
    )
    input_grad = input_sum.astype(jnp.bfloat16).reshape((1,) + input_sum.shape)
    return (query_grad, key_grad, input_grad, weight_grad)


def solution(mesh):
    groups, ranks = mesh.shape["dp"], mesh.shape["tensor"]

    def body(*operands):
        width = operands[0].shape[2]
        if width % (groups * ranks * 128) == 0:
            return fused_per_device(groups, ranks, *operands)
        return per_device(*operands)

    return jax.shard_map(
        body,
        mesh=mesh,
        in_specs=(
            P("dp", None, None),
            P(None, "tensor"),
            P("dp", None, "tensor"),
            P("dp", None, "tensor"),
            P("dp", None, "tensor"),
            P("dp", None, "tensor"),
            P("dp", None, "tensor"),
            P("dp", None),
        ),
        out_specs=(
            P("dp", None, "tensor"),
            P("dp", None, "tensor"),
            P("dp", "tensor", None),
            P("dp", "tensor"),
        ),
        check_vma=False,
    )
```

```python
import functools
import math

import jax
import jax.numpy as jnp
from jax import lax
from jax.experimental import pallas as pl
from jax.experimental.pallas import tpu as pltpu
from jax.sharding import PartitionSpec as P

MESH = pl.DeviceIdType.MESH
F32 = jnp.float32
BF16 = jnp.bfloat16
NT = (((1,), (1,)), ((), ()))


def fused(
    groups,
    ranks,
    hidden_hbm,
    weight_hbm,
    queries_hbm,
    key_ref,
    out_hbm,
    grad_hbm,
    norm_hbm,
    doc_hbm,
    qg_ref,
    kg_ref,
    ig_ref,
    wg_ref,
    hidden,
    weight,
    queries_ref,
    out_ref,
    grad_ref,
    norm_ref,
    doc_ref,
    piece,
    keys_t,
    values_t,
    probs,
    part,
    got_part,
    grads_t,
    out_buf,
    core_send,
    core_got,
    chip_send,
    chip_got,
    load_sem,
    pair_send,
    pair_recv,
    wa_send,
    wa_recv,
    wb_send,
    wb_recv,
    fw_send,
    vg_send,
    vg_recv,
    dc_send,
    dc_recv,
    dx_send,
    dx_recv,
    o_send,
    o_recv,
):
    d = lax.axis_index("dp")
    t = lax.axis_index("tensor")
    member = t % 2
    pair = t + 1 - 2 * member
    core = d % 2
    chip = d // 2
    other_core = d + 1 - 2 * core
    chips = groups // 2
    tokens, width = hidden.shape
    half = weight.shape[0]
    heads = norm_ref.shape[0]
    hd = 2 * half
    scale = 1.0 / math.sqrt(hd)
    span = width // ranks
    sub = span // groups
    rows = tokens // ranks
    wg_cols = width // groups

    def ds(index, size):
        return pl.ds(pl.multiple_of(index * size, size), size)

    def remote(src, dst, send, recv, **device):
        return pltpu.make_async_remote_copy(
            src_ref=src, dst_ref=dst, send_sem=send, recv_sem=recv,
            device_id=device, device_id_type=MESH,
        )

    started = []

    def send(src, dst, ssem, rsem, **device):
        copy = remote(src, dst, ssem, rsem, **device)
        copy.start()
        started.append(copy)

    load_w = pltpu.make_async_copy(weight_hbm, weight, load_sem.at[0])
    load_h = pltpu.make_async_copy(hidden_hbm, hidden, load_sem.at[1])
    load_p = pltpu.make_async_copy(
        weight_hbm.at[:, ds(t, span)], piece.at[ds(t, half), :], load_sem.at[2]
    )
    load_k = pltpu.make_async_copy(key_ref, keys_t.at[member], load_sem.at[3])
    load_g = pltpu.make_async_copy(grad_hbm, grad_ref, load_sem.at[4])
    load_o = pltpu.make_async_copy(out_hbm, out_ref, load_sem.at[5])
    load_q = pltpu.make_async_copy(queries_hbm, queries_ref, load_sem.at[6])
    load_n = pltpu.make_async_copy(norm_hbm, norm_ref, load_sem.at[7])
    load_d = pltpu.make_async_copy(doc_hbm, doc_ref, load_sem.at[8])
    for load in (load_k, load_d, load_n, load_g, load_o, load_q, load_w, load_h, load_p):
        load.start()

    barrier = pltpu.get_barrier_semaphore()
    for r in range(1, ranks):
        pl.semaphore_signal(barrier, inc=1, device_id={"tensor": (t + r) % ranks}, device_id_type=MESH)
    for i in range(1, groups):
        pl.semaphore_signal(barrier, inc=1, device_id={"dp": (d + i) % groups}, device_id_type=MESH)
    pl.semaphore_wait(barrier, ranks + groups - 2)

    send(key_ref, keys_t.at[member], pair_send.at[0], pair_recv.at[0], tensor=pair)
    for r in range(1, ranks):
        to = (t + r) % ranks
        send(
            weight_hbm.at[:, ds(to * groups + d, sub)],
            piece.at[ds(t, half), ds(d, sub)],
            wa_send.at[to], wa_recv.at[t], tensor=to,
        )

    load_g.wait()
    load_o.wait()
    load_d.wait()
    lane = lax.broadcasted_iota(jnp.int32, (tokens, hd), 1)
    dots = jnp.zeros((tokens, hd), F32)
    for j in range(heads):
        cols = slice(j * hd, (j + 1) * hd)
        product = grad_ref[:, cols].astype(F32) * out_ref[:, cols].astype(F32)
        dots = jnp.where(lane == j, jnp.sum(product, axis=1, keepdims=True), dots)
    dots = dots.T
    doc_row = jnp.broadcast_to(doc_ref[...].astype(F32), (tokens, tokens))
    doc_col = doc_row.T
    s_index = lax.broadcasted_iota(jnp.int32, (tokens, tokens), 0)
    t_index = lax.broadcasted_iota(jnp.int32, (tokens, tokens), 1)
    allowed = (s_index <= t_index) & (doc_row == doc_col)

    load_k.wait()
    load_q.wait()
    load_n.wait()
    remote(key_ref, keys_t.at[1 - member], pair_send.at[0], pair_recv.at[0], tensor=pair).wait_recv()
    keys = keys_t[...].reshape(hd, tokens).astype(F32).T.astype(BF16)
    total = jnp.zeros((tokens, hd), F32)
    for j in range(heads):
        cols = slice(j * hd, (j + 1) * hd)
        scores = lax.dot_general(keys, queries_ref[:, cols], NT, preferred_element_type=F32) * scale
        prob = jnp.where(allowed, jnp.exp(scores - norm_ref[j : j + 1, :]), 0.0)
        probs[j] = prob
        total += jnp.dot(prob.astype(BF16), grad_ref[:, cols], preferred_element_type=F32)
    part[0] = total.T
    send(
        part.at[0, ds(1 - member, half), :], got_part.at[0],
        pair_send.at[1], pair_recv.at[1], tensor=pair,
    )

    for r in range(1, ranks):
        source = (t + r) % ranks
        block = piece.at[ds(source, half), ds(d, sub)]
        remote(block, block, wa_send.at[source], wa_recv.at[source], tensor=source).wait_recv()
        for to in [other_core] + [(chip + i) % chips * 2 + core for i in range(1, chips)]:
            send(block, block, wb_send.at[source, to], wb_recv.at[source, d], dp=to)

    load_w.wait()
    load_h.wait()
    chunk = wg_cols
    value = jnp.zeros((half, tokens), F32)
    for c in range(width // chunk):
        cols = slice(c * chunk, (c + 1) * chunk)
        value += lax.dot_general(weight[:, cols], hidden[:, cols], NT, preferred_element_type=F32)
    values_t[member] = value.astype(BF16)
    send(values_t.at[member], values_t.at[member], pair_send.at[2], pair_recv.at[2], tensor=pair)

    remote(got_part.at[0], got_part.at[0], pair_send.at[1], pair_recv.at[1], tensor=pair).wait_recv()
    grad_own = (part[0, ds(member, half), :] + got_part[0]).astype(BF16)
    grads_t[ds(t, half), :] = grad_own
    for r in range(1, ranks):
        to = (t + r) % ranks
        block = grads_t.at[ds(t, half), :]
        send(block, block, vg_send.at[to], vg_recv.at[t], tensor=to)

    def partial_wg(owner):
        return jnp.dot(grad_own, hidden[:, ds(owner, wg_cols)], preferred_element_type=F32)

    for i in range(chips):
        c = (chip + 1 + i) % chips
        core_send[i] = partial_wg(c * 2 + 1 - core).astype(BF16)
        send(core_send.at[i], core_got.at[i], dc_send.at[i], dc_recv.at[i], dp=other_core)

    for r in range(1, ranks):
        source = (t + r) % ranks
        block = grads_t.at[ds(source, half), :]
        remote(block, block, vg_send.at[source], vg_recv.at[source], tensor=source).wait_recv()
    grads = grads_t[...].astype(F32).T.astype(BF16)
    load_p.wait()

    order = [d, other_core]
    straight = [(chip + chips - i) % chips * 2 + core for i in range(1, chips)]
    for i in range(chips - 1):
        order.append(straight[i])
        if i:
            order.append(straight[i - 1] + 1 - 2 * core)
    order.append(straight[-1] + 1 - 2 * core)

    def arrive(i):
        g = order[i]
        for r in range(1, ranks):
            source = (t + r) % ranks
            block = piece.at[ds(source, half), ds(g, sub)]
            remote(block, block, wb_send.at[source, g], wb_recv.at[source, g], dp=other_core).wait_recv()
            if any(g is s for s in straight):
                send(block, block, fw_send.at[source, g], wb_recv.at[source, g], dp=other_core)

    def input_chunk(i):
        g = order[i]
        if i:
            arrive(i)
        out_buf[i] = jnp.dot(grads, piece[:, ds(g, sub)], preferred_element_type=F32).astype(BF16)
        place = ds(t * groups + g, sub)
        for r in range(1, ranks):
            to = (t + r) % ranks
            send(
                out_buf.at[i, ds(to, rows), :], ig_ref.at[:, place],
                o_send.at[to, g], o_recv.at[t, g], tensor=to,
            )
        ig_ref[:, place] = out_buf[i, ds(t, rows), :]

    input_chunk(0)

    for i in range(chips):
        remote(core_send.at[i], core_got.at[i], dc_send.at[i], dc_recv.at[i], dp=other_core).wait_recv()
        if i < chips - 1:
            c = (chip + 1 + i) % chips
            chip_send[i] = (partial_wg(c * 2 + core) + core_got[i].astype(F32)).astype(BF16)
            send(chip_send.at[i], chip_got.at[i], dx_send.at[i], dx_recv.at[i], dp=c * 2 + core)
    wg_ref[...] = partial_wg(d) + core_got[chips - 1].astype(F32)

    input_chunk(1)
    input_chunk(2)

    remote(values_t.at[1 - member], values_t.at[1 - member], pair_send.at[2], pair_recv.at[2], tensor=pair).wait_recv()
    values = values_t[...].reshape(hd, tokens).astype(F32).T.astype(BF16)
    total = jnp.zeros((tokens, hd), F32)
    for j in range(heads):
        cols = slice(j * hd, (j + 1) * hd)
        prob_grad = lax.dot_general(values, grad_ref[:, cols], NT, preferred_element_type=F32)
        score_grad = probs[j] * (prob_grad - dots[j : j + 1, :]) * scale
        total += jnp.dot(score_grad.astype(BF16), queries_ref[:, cols], preferred_element_type=F32)
        qg_ref[:, cols] = jnp.dot(
            score_grad.T.astype(BF16), keys, preferred_element_type=F32
        ).astype(BF16)
    part[1] = total.T
    send(
        part.at[1, ds(1 - member, half), :], got_part.at[1],
        pair_send.at[3], pair_recv.at[3], tensor=pair,
    )

    for i in range(3, groups):
        input_chunk(i)

    remote(got_part.at[1], got_part.at[1], pair_send.at[3], pair_recv.at[3], tensor=pair).wait_recv()
    kg_ref[...] = (part[1, ds(member, half), :] + got_part[1]).astype(BF16)

    for i in range(chips - 1):
        c = (chip + chips - 1 - i) % chips
        remote(chip_send.at[i], chip_got.at[i], dx_send.at[i], dx_recv.at[i], dp=c * 2 + core).wait_recv()
        wg_ref[...] += chip_got[i].astype(F32)

    for r in range(1, ranks):
        source = (t + r) % ranks
        for i in range(groups):
            g = (d + groups - i) % groups
            place = ig_ref.at[:, ds(source * groups + g, sub)]
            remote(
                out_buf.at[0, ds(source, rows), :], place,
                o_send.at[source, g], o_recv.at[source, g], tensor=source,
            ).wait_recv()
    for copy in started:
        copy.wait_send()


def write_out(*refs):
    count = len(refs) // 2
    sems = refs[-1]
    copies = [
        pltpu.make_async_copy(refs[i], refs[count + i], sems.at[i]) for i in range(count)
    ]
    for copy in copies:
        copy.start()
    for copy in copies:
        copy.wait()


def fused_per_device(groups, ranks, hidden_in, value_weight, queries, key_rows, attention_out,
                     output_grad, log_normalizer, document_ids):
    _, tokens, width = hidden_in.shape
    half = value_weight.shape[1]
    hd = 2 * half
    heads = log_normalizer.shape[2]
    span = width // ranks
    sub = span // groups
    chips = groups // 2
    wg_cols = width // groups
    vmem = pl.BlockSpec(memory_space=pltpu.VMEM)
    hbm = pl.BlockSpec(memory_space=pltpu.HBM)
    sem = pltpu.SemaphoreType.DMA
    query_grad, key_grad, input_grad, weight_grad = pl.pallas_call(
        functools.partial(fused, groups, ranks),
        out_shape=(
            jax.ShapeDtypeStruct((tokens, heads * hd), BF16),
            jax.ShapeDtypeStruct((half, tokens), BF16),
            jax.ShapeDtypeStruct((tokens // ranks, width), BF16),
            jax.ShapeDtypeStruct((half, wg_cols), F32),
        ),
        in_specs=[hbm] * 8,
        out_specs=(vmem,) * 4,
        scratch_shapes=[
            pltpu.VMEM((tokens, width), BF16),
            pltpu.VMEM((half, width), BF16),
            pltpu.VMEM((tokens, heads * hd), BF16),
            pltpu.VMEM((tokens, heads * hd), BF16),
            pltpu.VMEM((tokens, heads * hd), BF16),
            pltpu.VMEM((heads, tokens), F32),
            pltpu.VMEM((1, tokens), jnp.int32),
            pltpu.VMEM((ranks * half, span), BF16),
            pltpu.VMEM((2, half, tokens), BF16),
            pltpu.VMEM((2, half, tokens), BF16),
            pltpu.VMEM((heads, tokens, tokens), F32),
            pltpu.VMEM((2, hd, tokens), F32),
            pltpu.VMEM((2, half, tokens), F32),
            pltpu.VMEM((ranks * half, tokens), BF16),
            pltpu.VMEM((groups, tokens, sub), BF16),
            pltpu.VMEM((chips, half, wg_cols), BF16),
            pltpu.VMEM((chips, half, wg_cols), BF16),
            pltpu.VMEM((chips - 1, half, wg_cols), BF16),
            pltpu.VMEM((chips - 1, half, wg_cols), BF16),
            sem((9,)),
            sem((4,)),
            sem((4,)),
            sem((ranks,)),
            sem((ranks,)),
            sem((ranks, groups)),
            sem((ranks, groups)),
            sem((ranks, groups)),
            sem((ranks,)),
            sem((ranks,)),
            sem((chips,)),
            sem((chips,)),
            sem((chips,)),
            sem((chips,)),
            sem((ranks, groups)),
            sem((ranks, groups)),
        ],
        compiler_params=pltpu.CompilerParams(
            collective_id=0, has_side_effects=True, vmem_limit_bytes=56 * 1024 * 1024
        ),
    )(
        hidden_in[0],
        value_weight.T,
        queries[0],
        key_rows[0].T,
        attention_out[0],
        output_grad[0],
        log_normalizer[0].T,
        document_ids,
    )
    results = (query_grad, key_grad, input_grad, weight_grad)
    query_grad, key_grad, input_grad, weight_grad = pl.pallas_call(
        write_out,
        out_shape=tuple(jax.ShapeDtypeStruct(x.shape, x.dtype) for x in results),
        in_specs=[vmem] * len(results),
        out_specs=(hbm,) * len(results),
        scratch_shapes=[sem((len(results),))],
    )(*results)
    return query_grad[None], key_grad.T[None], input_grad[None], weight_grad.T


def partner(value, axis, distance):
    mask = 2**distance
    pairs = [(source, source ^ mask) for source in range(lax.axis_size(axis))]
    return lax.ppermute(value, axis, pairs)


def per_device(
    hidden_in,
    value_weight,
    queries,
    key_rows,
    attention_out,
    output_grad,
    log_normalizer,
    document_ids,
):
    tokens = hidden_in.shape[1]
    head_count = log_normalizer.shape[2]
    half_width = key_rows.shape[2]
    head_width = 2 * half_width
    score_scale = 1.0 / math.sqrt(head_width)
    inputs_local = hidden_in[0]
    value_half = jnp.dot(inputs_local, value_weight, preferred_element_type=jnp.float32).astype(
        jnp.bfloat16
    )
    key_half = key_rows[0]
    other_key, other_value = partner((key_half, value_half), "tensor", 0)
    pair_member = lax.axis_index("tensor") % 2
    lower_member = pair_member == 0
    keys_full = jnp.where(
        lower_member,
        jnp.concatenate([key_half, other_key], 1),
        jnp.concatenate([other_key, key_half], 1),
    )
    values_full = jnp.where(
        lower_member,
        jnp.concatenate([value_half, other_value], 1),
        jnp.concatenate([other_value, value_half], 1),
    )
    query_heads = queries[0].reshape(tokens, head_count, head_width)
    grad_heads = output_grad[0].reshape(tokens, head_count, head_width)
    out_heads = attention_out[0].reshape(tokens, head_count, head_width)
    position = jnp.arange(tokens, dtype=jnp.int32)
    documents = document_ids[0]
    allowed = (position[None, :] <= position[:, None]) & (documents[:, None] == documents[None, :])
    scores = (
        jnp.einsum("thd,sd->hts", query_heads, keys_full, preferred_element_type=jnp.float32)
        * score_scale
    )
    normalizers = jnp.transpose(log_normalizer[0])[:, :, None]
    probabilities = jnp.where(allowed[None], jnp.exp(scores - normalizers), 0.0)
    probs_low = probabilities.astype(jnp.bfloat16)
    value_part = jnp.einsum(
        "hts,thd->sd", probs_low, grad_heads, preferred_element_type=jnp.float32
    )
    row_dots = jnp.einsum("thd,thd->ht", grad_heads, out_heads, preferred_element_type=jnp.float32)
    prob_grad = jnp.einsum(
        "thd,sd->hts", grad_heads, values_full, preferred_element_type=jnp.float32
    )
    score_grad = (probabilities * (prob_grad - row_dots[:, :, None]) * score_scale).astype(
        jnp.bfloat16
    )
    query_grad = jnp.einsum(
        "hts,sd->thd", score_grad, keys_full, preferred_element_type=jnp.float32
    )
    query_grad = query_grad.astype(jnp.bfloat16).reshape(1, tokens, head_count * head_width)
    key_part = jnp.einsum(
        "hts,thd->sd", score_grad, query_heads, preferred_element_type=jnp.float32
    )
    own_offset = pair_member * half_width
    other_offset = (1 - pair_member) * half_width
    send_key = lax.dynamic_slice_in_dim(key_part, other_offset, half_width, 1)
    send_value = lax.dynamic_slice_in_dim(value_part, other_offset, half_width, 1)
    got_key, got_value = partner((send_key, send_value), "tensor", 0)
    key_sum = lax.dynamic_slice_in_dim(key_part, own_offset, half_width, 1) + got_key
    value_sum = lax.dynamic_slice_in_dim(value_part, own_offset, half_width, 1) + got_value
    key_grad = key_sum.astype(jnp.bfloat16).reshape(1, tokens, half_width)
    value_grad = value_sum.astype(jnp.bfloat16)
    input_sum = lax.psum_scatter(
        lax.dot_general(
            value_grad, value_weight, (((1,), (1,)), ((), ())), preferred_element_type=jnp.float32
        ).astype(jnp.bfloat16),
        "tensor",
        scatter_dimension=0,
        tiled=True,
    ).astype(jnp.float32)
    weight_grad = lax.psum_scatter(
        lax.dot_general(
            inputs_local, value_grad, (((0,), (0,)), ((), ())), preferred_element_type=jnp.float32
        ),
        "dp",
        scatter_dimension=0,
        tiled=True,
    )
    input_grad = input_sum.astype(jnp.bfloat16).reshape((1,) + input_sum.shape)
    return (query_grad, key_grad, input_grad, weight_grad)


def solution(mesh):
    groups, ranks = mesh.shape["dp"], mesh.shape["tensor"]

    def body(*operands):
        width = operands[0].shape[2]
        if width % (groups * ranks * 128) == 0:
            return fused_per_device(groups, ranks, *operands)
        return per_device(*operands)

    return jax.shard_map(
        body,
        mesh=mesh,
        in_specs=(
            P("dp", None, None),
            P(None, "tensor"),
            P("dp", None, "tensor"),
            P("dp", None, "tensor"),
            P("dp", None, "tensor"),
            P("dp", None, "tensor"),
            P("dp", None, "tensor"),
            P("dp", None),
        ),
        out_specs=(
            P("dp", None, "tensor"),
            P("dp", None, "tensor"),
            P("dp", "tensor", None),
            P("dp", "tensor"),
        ),
        check_vma=False,
    )
```

```python
import functools
import math

import jax
import jax.numpy as jnp
from jax import lax
from jax.experimental import pallas as pl
from jax.experimental.pallas import tpu as pltpu
from jax.sharding import PartitionSpec as P

MESH = pl.DeviceIdType.MESH
F32 = jnp.float32
BF16 = jnp.bfloat16
NT = (((1,), (1,)), ((), ()))


def fused(
    groups,
    ranks,
    hidden_hbm,
    weight_hbm,
    queries_hbm,
    key_ref,
    out_hbm,
    grad_hbm,
    norm_hbm,
    doc_hbm,
    qg_ref,
    kg_ref,
    ig_ref,
    wg_ref,
    hidden,
    weight,
    queries_ref,
    out_ref,
    grad_ref,
    norm_ref,
    doc_ref,
    piece,
    keys_t,
    values_t,
    probs,
    part,
    got_part,
    grads_t,
    grads_ref,
    out_buf,
    core_send,
    core_got,
    chip_send,
    chip_got,
    load_sem,
    pair_send,
    pair_recv,
    wa_send,
    wa_recv,
    wb_send,
    wb_recv,
    fw_send,
    vg_send,
    vg_recv,
    dc_send,
    dc_recv,
    dx_send,
    dx_recv,
    o_send,
    o_recv,
):
    d = lax.axis_index("dp")
    t = lax.axis_index("tensor")
    member = t % 2
    pair = t + 1 - 2 * member
    core = d % 2
    chip = d // 2
    other_core = d + 1 - 2 * core
    chips = groups // 2
    tokens, width = hidden.shape
    half = weight.shape[0]
    heads = norm_ref.shape[0]
    hd = 2 * half
    scale = 1.0 / math.sqrt(hd)
    span = width // 2
    sub = span // groups
    rows = tokens // ranks
    wg_cols = width // groups

    def ds(index, size):
        return pl.ds(pl.multiple_of(index * size, size), size)

    def remote(src, dst, send, recv, **device):
        return pltpu.make_async_remote_copy(
            src_ref=src, dst_ref=dst, send_sem=send, recv_sem=recv,
            device_id=device, device_id_type=MESH,
        )

    started = []

    def send(src, dst, ssem, rsem, **device):
        copy = remote(src, dst, ssem, rsem, **device)
        copy.start()
        started.append(copy)

    load_w = pltpu.make_async_copy(weight_hbm, weight, load_sem.at[0])
    load_h = pltpu.make_async_copy(hidden_hbm, hidden, load_sem.at[1])
    load_p = pltpu.make_async_copy(
        weight_hbm.at[:, ds(member, span)], piece.at[ds(t, half), :], load_sem.at[2]
    )
    load_k = pltpu.make_async_copy(key_ref, keys_t.at[member], load_sem.at[3])
    load_g = pltpu.make_async_copy(grad_hbm, grad_ref, load_sem.at[4])
    load_o = pltpu.make_async_copy(out_hbm, out_ref, load_sem.at[5])
    load_q = pltpu.make_async_copy(queries_hbm, queries_ref, load_sem.at[6])
    load_n = pltpu.make_async_copy(norm_hbm, norm_ref, load_sem.at[7])
    load_d = pltpu.make_async_copy(doc_hbm, doc_ref, load_sem.at[8])
    for load in (load_k, load_d, load_n, load_g, load_o, load_q, load_w, load_h, load_p):
        load.start()

    barrier = pltpu.get_barrier_semaphore()
    for r in range(1, ranks):
        pl.semaphore_signal(barrier, inc=1, device_id={"tensor": (t + r) % ranks}, device_id_type=MESH)
    for i in range(1, groups):
        pl.semaphore_signal(barrier, inc=1, device_id={"dp": (d + i) % groups}, device_id_type=MESH)
    pl.semaphore_wait(barrier, ranks + groups - 2)

    send(key_ref, keys_t.at[member], pair_send.at[0], pair_recv.at[0], tensor=pair)
    for r in range(1, ranks):
        to = (t + r) % ranks
        send(
            weight_hbm.at[:, ds(to % 2 * groups + d, sub)],
            piece.at[ds(t, half), ds(d, sub)],
            wa_send.at[to], wa_recv.at[t], tensor=to,
        )

    load_g.wait()
    load_o.wait()
    load_d.wait()
    lane = lax.broadcasted_iota(jnp.int32, (tokens, hd), 1)
    dots = jnp.zeros((tokens, hd), F32)
    for j in range(heads):
        cols = slice(j * hd, (j + 1) * hd)
        product = grad_ref[:, cols].astype(F32) * out_ref[:, cols].astype(F32)
        dots = jnp.where(lane == j, jnp.sum(product, axis=1, keepdims=True), dots)
    dots = dots.T
    doc_row = jnp.broadcast_to(doc_ref[...].astype(F32), (tokens, tokens))
    doc_col = doc_row.T
    s_index = lax.broadcasted_iota(jnp.int32, (tokens, tokens), 0)
    t_index = lax.broadcasted_iota(jnp.int32, (tokens, tokens), 1)
    allowed = (s_index <= t_index) & (doc_row == doc_col)

    load_k.wait()
    load_q.wait()
    load_n.wait()
    remote(key_ref, keys_t.at[1 - member], pair_send.at[0], pair_recv.at[0], tensor=pair).wait_recv()
    keys = keys_t[...].reshape(hd, tokens).astype(F32).T.astype(BF16)
    total = jnp.zeros((tokens, hd), F32)
    for j in range(heads):
        cols = slice(j * hd, (j + 1) * hd)
        scores = lax.dot_general(keys, queries_ref[:, cols], NT, preferred_element_type=F32) * scale
        prob = jnp.where(allowed, jnp.exp(scores - norm_ref[j : j + 1, :]), 0.0)
        probs[j] = prob
        total += jnp.dot(prob.astype(BF16), grad_ref[:, cols], preferred_element_type=F32)
    part[0] = total.T
    send(
        part.at[0, ds(1 - member, half), :], got_part.at[0],
        pair_send.at[1], pair_recv.at[1], tensor=pair,
    )

    for r in range(1, ranks):
        source = (t + r) % ranks
        block = piece.at[ds(source, half), ds(d, sub)]
        remote(block, block, wa_send.at[source], wa_recv.at[source], tensor=source).wait_recv()
        for to in [other_core] + [(chip + i) % chips * 2 + core for i in range(1, chips)]:
            send(block, block, wb_send.at[source, to], wb_recv.at[source, d], dp=to)

    load_w.wait()
    load_h.wait()
    chunk = wg_cols
    value = jnp.zeros((half, tokens), F32)
    for c in range(width // chunk):
        cols = slice(c * chunk, (c + 1) * chunk)
        value += lax.dot_general(weight[:, cols], hidden[:, cols], NT, preferred_element_type=F32)
    values_t[member] = value.astype(BF16)
    send(values_t.at[member], values_t.at[member], pair_send.at[2], pair_recv.at[2], tensor=pair)

    remote(got_part.at[0], got_part.at[0], pair_send.at[1], pair_recv.at[1], tensor=pair).wait_recv()
    grad_own = (part[0, ds(member, half), :] + got_part[0]).astype(BF16)
    grads_t[ds(t, half), :] = grad_own
    for r in range(1, ranks):
        to = (t + r) % ranks
        block = grads_t.at[ds(t, half), :]
        send(block, block, vg_send.at[to], vg_recv.at[t], tensor=to)

    def partial_wg(owner):
        return jnp.dot(grad_own, hidden[:, ds(owner, wg_cols)], preferred_element_type=F32)

    for i in range(chips):
        c = (chip + 1 + i) % chips
        core_send[i] = partial_wg(c * 2 + 1 - core).astype(BF16)
        send(core_send.at[i], core_got.at[i], dc_send.at[i], dc_recv.at[i], dp=other_core)

    for r in range(1, ranks):
        source = (t + r) % ranks
        block = grads_t.at[ds(source, half), :]
        remote(block, block, vg_send.at[source], vg_recv.at[source], tensor=source).wait_recv()
    grads_ref[...] = grads_t[...].astype(F32).T.astype(BF16)
    grads = grads_ref[ds(t // 2, 2 * rows), :]
    load_p.wait()

    order = [d, other_core]
    straight = [(chip + chips - i) % chips * 2 + core for i in range(1, chips)]
    for i in range(chips - 1):
        order.append(straight[i])
        if i:
            order.append(straight[i - 1] + 1 - 2 * core)
    order.append(straight[-1] + 1 - 2 * core)

    def arrive(i):
        g = order[i]
        for r in range(1, ranks):
            source = (t + r) % ranks
            block = piece.at[ds(source, half), ds(g, sub)]
            remote(block, block, wb_send.at[source, g], wb_recv.at[source, g], dp=other_core).wait_recv()
            if any(g is s for s in straight):
                send(block, block, fw_send.at[source, g], wb_recv.at[source, g], dp=other_core)

    def input_chunk(i):
        g = order[i]
        if i:
            arrive(i)
        out_buf[i] = jnp.dot(grads, piece[:, ds(g, sub)], preferred_element_type=F32).astype(BF16)
        place = ds(member * groups + g, sub)
        send(
            out_buf.at[i, ds(1 - member, rows), :], ig_ref.at[:, place],
            o_send.at[g], o_recv.at[g], tensor=pair,
        )
        ig_ref[:, place] = out_buf[i, ds(member, rows), :]

    input_chunk(0)

    for i in range(chips):
        remote(core_send.at[i], core_got.at[i], dc_send.at[i], dc_recv.at[i], dp=other_core).wait_recv()
        if i < chips - 1:
            c = (chip + 1 + i) % chips
            chip_send[i] = (partial_wg(c * 2 + core) + core_got[i].astype(F32)).astype(BF16)
            send(chip_send.at[i], chip_got.at[i], dx_send.at[i], dx_recv.at[i], dp=c * 2 + core)
    wg_ref[...] = partial_wg(d) + core_got[chips - 1].astype(F32)

    input_chunk(1)
    input_chunk(2)

    remote(values_t.at[1 - member], values_t.at[1 - member], pair_send.at[2], pair_recv.at[2], tensor=pair).wait_recv()
    values = values_t[...].reshape(hd, tokens).astype(F32).T.astype(BF16)
    total = jnp.zeros((tokens, hd), F32)
    for j in range(heads):
        cols = slice(j * hd, (j + 1) * hd)
        prob_grad = lax.dot_general(values, grad_ref[:, cols], NT, preferred_element_type=F32)
        score_grad = probs[j] * (prob_grad - dots[j : j + 1, :]) * scale
        total += jnp.dot(score_grad.astype(BF16), queries_ref[:, cols], preferred_element_type=F32)
        qg_ref[:, cols] = jnp.dot(
            score_grad.T.astype(BF16), keys, preferred_element_type=F32
        ).astype(BF16)
    part[1] = total.T
    send(
        part.at[1, ds(1 - member, half), :], got_part.at[1],
        pair_send.at[3], pair_recv.at[3], tensor=pair,
    )

    for i in range(3, groups):
        input_chunk(i)

    remote(got_part.at[1], got_part.at[1], pair_send.at[3], pair_recv.at[3], tensor=pair).wait_recv()
    kg_ref[...] = (part[1, ds(member, half), :] + got_part[1]).astype(BF16)

    for i in range(chips - 1):
        c = (chip + chips - 1 - i) % chips
        remote(chip_send.at[i], chip_got.at[i], dx_send.at[i], dx_recv.at[i], dp=c * 2 + core).wait_recv()
        wg_ref[...] += chip_got[i].astype(F32)

    for g in order:
        place = ig_ref.at[:, ds((1 - member) * groups + g, sub)]
        remote(
            out_buf.at[0, ds(member, rows), :], place, o_send.at[g], o_recv.at[g], tensor=pair
        ).wait_recv()
    for copy in started:
        copy.wait_send()


def write_out(*refs):
    count = len(refs) // 2
    sems = refs[-1]
    copies = [
        pltpu.make_async_copy(refs[i], refs[count + i], sems.at[i]) for i in range(count)
    ]
    for copy in copies:
        copy.start()
    for copy in copies:
        copy.wait()


def fused_per_device(groups, ranks, hidden_in, value_weight, queries, key_rows, attention_out,
                     output_grad, log_normalizer, document_ids):
    _, tokens, width = hidden_in.shape
    half = value_weight.shape[1]
    hd = 2 * half
    heads = log_normalizer.shape[2]
    span = width // 2
    sub = span // groups
    chips = groups // 2
    wg_cols = width // groups
    vmem = pl.BlockSpec(memory_space=pltpu.VMEM)
    hbm = pl.BlockSpec(memory_space=pltpu.HBM)
    sem = pltpu.SemaphoreType.DMA
    query_grad, key_grad, input_grad, weight_grad = pl.pallas_call(
        functools.partial(fused, groups, ranks),
        out_shape=(
            jax.ShapeDtypeStruct((tokens, heads * hd), BF16),
            jax.ShapeDtypeStruct((half, tokens), BF16),
            jax.ShapeDtypeStruct((tokens // ranks, width), BF16),
            jax.ShapeDtypeStruct((half, wg_cols), F32),
        ),
        in_specs=[hbm] * 8,
        out_specs=(vmem,) * 4,
        scratch_shapes=[
            pltpu.VMEM((tokens, width), BF16),
            pltpu.VMEM((half, width), BF16),
            pltpu.VMEM((tokens, heads * hd), BF16),
            pltpu.VMEM((tokens, heads * hd), BF16),
            pltpu.VMEM((tokens, heads * hd), BF16),
            pltpu.VMEM((heads, tokens), F32),
            pltpu.VMEM((1, tokens), jnp.int32),
            pltpu.VMEM((ranks * half, span), BF16),
            pltpu.VMEM((2, half, tokens), BF16),
            pltpu.VMEM((2, half, tokens), BF16),
            pltpu.VMEM((heads, tokens, tokens), F32),
            pltpu.VMEM((2, hd, tokens), F32),
            pltpu.VMEM((2, half, tokens), F32),
            pltpu.VMEM((ranks * half, tokens), BF16),
            pltpu.VMEM((tokens, ranks * half), BF16),
            pltpu.VMEM((groups, 2 * (tokens // ranks), sub), BF16),
            pltpu.VMEM((chips, half, wg_cols), BF16),
            pltpu.VMEM((chips, half, wg_cols), BF16),
            pltpu.VMEM((chips - 1, half, wg_cols), BF16),
            pltpu.VMEM((chips - 1, half, wg_cols), BF16),
            sem((9,)),
            sem((4,)),
            sem((4,)),
            sem((ranks,)),
            sem((ranks,)),
            sem((ranks, groups)),
            sem((ranks, groups)),
            sem((ranks, groups)),
            sem((ranks,)),
            sem((ranks,)),
            sem((chips,)),
            sem((chips,)),
            sem((chips,)),
            sem((chips,)),
            sem((groups,)),
            sem((groups,)),
        ],
        compiler_params=pltpu.CompilerParams(
            collective_id=0, has_side_effects=True, vmem_limit_bytes=56 * 1024 * 1024
        ),
    )(
        hidden_in[0],
        value_weight.T,
        queries[0],
        key_rows[0].T,
        attention_out[0],
        output_grad[0],
        log_normalizer[0].T,
        document_ids,
    )
    results = (query_grad, key_grad, input_grad, weight_grad)
    query_grad, key_grad, input_grad, weight_grad = pl.pallas_call(
        write_out,
        out_shape=tuple(jax.ShapeDtypeStruct(x.shape, x.dtype) for x in results),
        in_specs=[vmem] * len(results),
        out_specs=(hbm,) * len(results),
        scratch_shapes=[sem((len(results),))],
    )(*results)
    return query_grad[None], key_grad.T[None], input_grad[None], weight_grad.T


def partner(value, axis, distance):
    mask = 2**distance
    pairs = [(source, source ^ mask) for source in range(lax.axis_size(axis))]
    return lax.ppermute(value, axis, pairs)


def per_device(
    hidden_in,
    value_weight,
    queries,
    key_rows,
    attention_out,
    output_grad,
    log_normalizer,
    document_ids,
):
    tokens = hidden_in.shape[1]
    head_count = log_normalizer.shape[2]
    half_width = key_rows.shape[2]
    head_width = 2 * half_width
    score_scale = 1.0 / math.sqrt(head_width)
    inputs_local = hidden_in[0]
    value_half = jnp.dot(inputs_local, value_weight, preferred_element_type=jnp.float32).astype(
        jnp.bfloat16
    )
    key_half = key_rows[0]
    other_key, other_value = partner((key_half, value_half), "tensor", 0)
    pair_member = lax.axis_index("tensor") % 2
    lower_member = pair_member == 0
    keys_full = jnp.where(
        lower_member,
        jnp.concatenate([key_half, other_key], 1),
        jnp.concatenate([other_key, key_half], 1),
    )
    values_full = jnp.where(
        lower_member,
        jnp.concatenate([value_half, other_value], 1),
        jnp.concatenate([other_value, value_half], 1),
    )
    query_heads = queries[0].reshape(tokens, head_count, head_width)
    grad_heads = output_grad[0].reshape(tokens, head_count, head_width)
    out_heads = attention_out[0].reshape(tokens, head_count, head_width)
    position = jnp.arange(tokens, dtype=jnp.int32)
    documents = document_ids[0]
    allowed = (position[None, :] <= position[:, None]) & (documents[:, None] == documents[None, :])
    scores = (
        jnp.einsum("thd,sd->hts", query_heads, keys_full, preferred_element_type=jnp.float32)
        * score_scale
    )
    normalizers = jnp.transpose(log_normalizer[0])[:, :, None]
    probabilities = jnp.where(allowed[None], jnp.exp(scores - normalizers), 0.0)
    probs_low = probabilities.astype(jnp.bfloat16)
    value_part = jnp.einsum(
        "hts,thd->sd", probs_low, grad_heads, preferred_element_type=jnp.float32
    )
    row_dots = jnp.einsum("thd,thd->ht", grad_heads, out_heads, preferred_element_type=jnp.float32)
    prob_grad = jnp.einsum(
        "thd,sd->hts", grad_heads, values_full, preferred_element_type=jnp.float32
    )
    score_grad = (probabilities * (prob_grad - row_dots[:, :, None]) * score_scale).astype(
        jnp.bfloat16
    )
    query_grad = jnp.einsum(
        "hts,sd->thd", score_grad, keys_full, preferred_element_type=jnp.float32
    )
    query_grad = query_grad.astype(jnp.bfloat16).reshape(1, tokens, head_count * head_width)
    key_part = jnp.einsum(
        "hts,thd->sd", score_grad, query_heads, preferred_element_type=jnp.float32
    )
    own_offset = pair_member * half_width
    other_offset = (1 - pair_member) * half_width
    send_key = lax.dynamic_slice_in_dim(key_part, other_offset, half_width, 1)
    send_value = lax.dynamic_slice_in_dim(value_part, other_offset, half_width, 1)
    got_key, got_value = partner((send_key, send_value), "tensor", 0)
    key_sum = lax.dynamic_slice_in_dim(key_part, own_offset, half_width, 1) + got_key
    value_sum = lax.dynamic_slice_in_dim(value_part, own_offset, half_width, 1) + got_value
    key_grad = key_sum.astype(jnp.bfloat16).reshape(1, tokens, half_width)
    value_grad = value_sum.astype(jnp.bfloat16)
    input_sum = lax.psum_scatter(
        lax.dot_general(
            value_grad, value_weight, (((1,), (1,)), ((), ())), preferred_element_type=jnp.float32
        ).astype(jnp.bfloat16),
        "tensor",
        scatter_dimension=0,
        tiled=True,
    ).astype(jnp.float32)
    weight_grad = lax.psum_scatter(
        lax.dot_general(
            inputs_local, value_grad, (((0,), (0,)), ((), ())), preferred_element_type=jnp.float32
        ),
        "dp",
        scatter_dimension=0,
        tiled=True,
    )
    input_grad = input_sum.astype(jnp.bfloat16).reshape((1,) + input_sum.shape)
    return (query_grad, key_grad, input_grad, weight_grad)


def solution(mesh):
    groups, ranks = mesh.shape["dp"], mesh.shape["tensor"]

    def body(*operands):
        width = operands[0].shape[2]
        if width % (groups * ranks * 128) == 0 and ranks % 2 == 0:
            return fused_per_device(groups, ranks, *operands)
        return per_device(*operands)

    return jax.shard_map(
        body,
        mesh=mesh,
        in_specs=(
            P("dp", None, None),
            P(None, "tensor"),
            P("dp", None, "tensor"),
            P("dp", None, "tensor"),
            P("dp", None, "tensor"),
            P("dp", None, "tensor"),
            P("dp", None, "tensor"),
            P("dp", None),
        ),
        out_specs=(
            P("dp", None, "tensor"),
            P("dp", None, "tensor"),
            P("dp", "tensor", None),
            P("dp", "tensor"),
        ),
        check_vma=False,
    )
```

```python
import functools
import math

import jax
import jax.numpy as jnp
from jax import lax
from jax.experimental import pallas as pl
from jax.experimental.pallas import tpu as pltpu
from jax.sharding import PartitionSpec as P

MESH = pl.DeviceIdType.MESH
F32 = jnp.float32
BF16 = jnp.bfloat16
NT = (((1,), (1,)), ((), ()))


def fused(
    groups,
    ranks,
    hidden_hbm,
    weight_hbm,
    queries_hbm,
    key_ref,
    out_hbm,
    grad_hbm,
    norm_hbm,
    doc_hbm,
    qg_ref,
    kg_ref,
    ig_ref,
    wg_ref,
    hidden,
    weight,
    queries_ref,
    out_ref,
    grad_ref,
    norm_ref,
    doc_ref,
    piece,
    keys_t,
    values_t,
    probs,
    part,
    got_part,
    grads_t,
    out_buf,
    core_send,
    core_got,
    chip_send,
    chip_got,
    load_sem,
    pair_send,
    pair_recv,
    wa_send,
    wa_recv,
    wb_send,
    wb_recv,
    fw_send,
    vg_send,
    vg_recv,
    dc_send,
    dc_recv,
    dx_send,
    dx_recv,
    o_send,
    o_recv,
):
    d = lax.axis_index("dp")
    t = lax.axis_index("tensor")
    member = t % 2
    pair = t + 1 - 2 * member
    core = d % 2
    chip = d // 2
    other_core = d + 1 - 2 * core
    chips = groups // 2
    tokens, width = hidden.shape
    half = weight.shape[0]
    heads = norm_ref.shape[0]
    hd = 2 * half
    scale = 1.0 / math.sqrt(hd)
    span = width // ranks
    sub = span // groups
    rows = tokens // ranks
    wg_cols = width // groups

    def ds(index, size):
        return pl.ds(pl.multiple_of(index * size, size), size)

    def remote(src, dst, send, recv, **device):
        return pltpu.make_async_remote_copy(
            src_ref=src, dst_ref=dst, send_sem=send, recv_sem=recv,
            device_id=device, device_id_type=MESH,
        )

    started = []

    def send(src, dst, ssem, rsem, **device):
        copy = remote(src, dst, ssem, rsem, **device)
        copy.start()
        started.append(copy)

    load_w = pltpu.make_async_copy(weight_hbm, weight, load_sem.at[0])
    load_h = pltpu.make_async_copy(hidden_hbm, hidden, load_sem.at[1])
    load_p = pltpu.make_async_copy(
        weight_hbm.at[:, ds(t, span)], piece.at[ds(t, half), :], load_sem.at[2]
    )
    load_k = pltpu.make_async_copy(key_ref, keys_t.at[member], load_sem.at[3])
    load_g = pltpu.make_async_copy(grad_hbm, grad_ref, load_sem.at[4])
    load_o = pltpu.make_async_copy(out_hbm, out_ref, load_sem.at[5])
    load_q = pltpu.make_async_copy(queries_hbm, queries_ref, load_sem.at[6])
    load_n = pltpu.make_async_copy(norm_hbm, norm_ref, load_sem.at[7])
    load_d = pltpu.make_async_copy(doc_hbm, doc_ref, load_sem.at[8])
    for load in (load_k, load_d, load_n, load_g, load_o, load_q, load_w, load_h, load_p):
        load.start()

    barrier = pltpu.get_barrier_semaphore()
    for r in range(1, ranks):
        pl.semaphore_signal(barrier, inc=1, device_id={"tensor": (t + r) % ranks}, device_id_type=MESH)
    for i in range(1, groups):
        pl.semaphore_signal(barrier, inc=1, device_id={"dp": (d + i) % groups}, device_id_type=MESH)
    pl.semaphore_wait(barrier, ranks + groups - 2)

    send(key_ref, keys_t.at[member], pair_send.at[0], pair_recv.at[0], tensor=pair)
    for r in range(1, ranks):
        to = (t + r) % ranks
        send(
            weight_hbm.at[:, ds(to * groups + d, sub)],
            piece.at[ds(t, half), ds(d, sub)],
            wa_send.at[to], wa_recv.at[t], tensor=to,
        )

    load_g.wait()
    load_o.wait()
    load_d.wait()
    lane = lax.broadcasted_iota(jnp.int32, (tokens, hd), 1)
    dots = jnp.zeros((tokens, hd), F32)
    for j in range(heads):
        cols = slice(j * hd, (j + 1) * hd)
        product = grad_ref[:, cols].astype(F32) * out_ref[:, cols].astype(F32)
        dots = jnp.where(lane == j, jnp.sum(product, axis=1, keepdims=True), dots)
    dots = dots.T
    doc_row = jnp.broadcast_to(doc_ref[...].astype(F32), (tokens, tokens))
    doc_col = doc_row.T
    s_index = lax.broadcasted_iota(jnp.int32, (tokens, tokens), 0)
    t_index = lax.broadcasted_iota(jnp.int32, (tokens, tokens), 1)
    allowed = (s_index <= t_index) & (doc_row == doc_col)

    load_k.wait()
    load_q.wait()
    load_n.wait()
    remote(key_ref, keys_t.at[1 - member], pair_send.at[0], pair_recv.at[0], tensor=pair).wait_recv()
    keys = keys_t[...].reshape(hd, tokens).astype(F32).T.astype(BF16)
    total = jnp.zeros((tokens, hd), F32)
    for j in range(heads):
        cols = slice(j * hd, (j + 1) * hd)
        scores = lax.dot_general(keys, queries_ref[:, cols], NT, preferred_element_type=F32) * scale
        prob = jnp.where(allowed, jnp.exp(scores - norm_ref[j : j + 1, :]), 0.0)
        probs[j] = prob
        total += jnp.dot(prob.astype(BF16), grad_ref[:, cols], preferred_element_type=F32)
    part[0] = total.T
    send(
        part.at[0, ds(1 - member, half), :], got_part.at[0],
        pair_send.at[1], pair_recv.at[1], tensor=pair,
    )

    for r in range(1, ranks):
        source = (t + r) % ranks
        block = piece.at[ds(source, half), ds(d, sub)]
        remote(block, block, wa_send.at[source], wa_recv.at[source], tensor=source).wait_recv()
        for to in [other_core] + [(chip + i) % chips * 2 + core for i in range(1, chips)]:
            send(block, block, wb_send.at[source, to], wb_recv.at[source, d], dp=to)

    load_w.wait()
    load_h.wait()
    chunk = wg_cols
    value = jnp.zeros((half, tokens), F32)
    for c in range(width // chunk):
        cols = slice(c * chunk, (c + 1) * chunk)
        value += lax.dot_general(weight[:, cols], hidden[:, cols], NT, preferred_element_type=F32)
    values_t[member] = value.astype(BF16)
    send(values_t.at[member], values_t.at[member], pair_send.at[2], pair_recv.at[2], tensor=pair)

    remote(got_part.at[0], got_part.at[0], pair_send.at[1], pair_recv.at[1], tensor=pair).wait_recv()
    grad_own = (part[0, ds(member, half), :] + got_part[0]).astype(BF16)
    grads_t[ds(t, half), :] = grad_own
    for r in range(1, ranks):
        to = (t + r) % ranks
        block = grads_t.at[ds(t, half), :]
        send(block, block, vg_send.at[to], vg_recv.at[t], tensor=to)

    def partial_wg(owner):
        return jnp.dot(grad_own, hidden[:, ds(owner, wg_cols)], preferred_element_type=F32)

    for i in range(chips):
        c = (chip + 1 + i) % chips
        core_send[i] = partial_wg(c * 2 + 1 - core).astype(BF16)
        send(core_send.at[i], core_got.at[i], dc_send.at[i], dc_recv.at[i], dp=other_core)

    for r in range(1, ranks):
        source = (t + r) % ranks
        block = grads_t.at[ds(source, half), :]
        remote(block, block, vg_send.at[source], vg_recv.at[source], tensor=source).wait_recv()
    grads = grads_t[...].astype(F32).T.astype(BF16)
    load_p.wait()

    order = [d, other_core]
    straight = [(chip + chips - i) % chips * 2 + core for i in range(1, chips)]
    for i in range(chips - 1):
        order.append(straight[i])
        if i:
            order.append(straight[i - 1] + 1 - 2 * core)
    order.append(straight[-1] + 1 - 2 * core)

    def arrive(i):
        g = order[i]
        for r in range(1, ranks):
            source = (t + r) % ranks
            block = piece.at[ds(source, half), ds(g, sub)]
            remote(block, block, wb_send.at[source, g], wb_recv.at[source, g], dp=other_core).wait_recv()
            if any(g is s for s in straight):
                send(block, block, fw_send.at[source, g], wb_recv.at[source, g], dp=other_core)

    def input_chunk(i):
        g = order[i]
        if i:
            arrive(i)
        out_buf[i] = jnp.dot(grads, piece[:, ds(g, sub)], preferred_element_type=F32).astype(BF16)
        place = ds(t * groups + g, sub)
        for r in range(1, ranks):
            to = (t + r) % ranks
            send(
                out_buf.at[i, ds(to, rows), :], ig_ref.at[:, place],
                o_send.at[to, g], o_recv.at[t, g], tensor=to,
            )
        ig_ref[:, place] = out_buf[i, ds(t, rows), :]

    input_chunk(0)

    for i in range(chips):
        remote(core_send.at[i], core_got.at[i], dc_send.at[i], dc_recv.at[i], dp=other_core).wait_recv()
        if i < chips - 1:
            c = (chip + 1 + i) % chips
            chip_send[i] = (partial_wg(c * 2 + core) + core_got[i].astype(F32)).astype(BF16)
            send(chip_send.at[i], chip_got.at[i], dx_send.at[i], dx_recv.at[i], dp=c * 2 + core)
    wg_ref[...] = partial_wg(d) + core_got[chips - 1].astype(F32)

    early = groups - 2
    for i in range(1, early):
        input_chunk(i)

    remote(values_t.at[1 - member], values_t.at[1 - member], pair_send.at[2], pair_recv.at[2], tensor=pair).wait_recv()
    values = values_t[...].reshape(hd, tokens).astype(F32).T.astype(BF16)
    total = jnp.zeros((tokens, hd), F32)
    for j in range(heads):
        cols = slice(j * hd, (j + 1) * hd)
        prob_grad = lax.dot_general(values, grad_ref[:, cols], NT, preferred_element_type=F32)
        score_grad = probs[j] * (prob_grad - dots[j : j + 1, :]) * scale
        total += jnp.dot(score_grad.astype(BF16), queries_ref[:, cols], preferred_element_type=F32)
        qg_ref[:, cols] = jnp.dot(
            score_grad.T.astype(BF16), keys, preferred_element_type=F32
        ).astype(BF16)
    part[1] = total.T
    send(
        part.at[1, ds(1 - member, half), :], got_part.at[1],
        pair_send.at[3], pair_recv.at[3], tensor=pair,
    )

    for i in range(early, groups):
        input_chunk(i)

    remote(got_part.at[1], got_part.at[1], pair_send.at[3], pair_recv.at[3], tensor=pair).wait_recv()
    kg_ref[...] = (part[1, ds(member, half), :] + got_part[1]).astype(BF16)

    for i in range(chips - 1):
        c = (chip + chips - 1 - i) % chips
        remote(chip_send.at[i], chip_got.at[i], dx_send.at[i], dx_recv.at[i], dp=c * 2 + core).wait_recv()
        wg_ref[...] += chip_got[i].astype(F32)

    for r in range(1, ranks):
        source = (t + r) % ranks
        for i in range(groups):
            g = (d + groups - i) % groups
            place = ig_ref.at[:, ds(source * groups + g, sub)]
            remote(
                out_buf.at[0, ds(source, rows), :], place,
                o_send.at[source, g], o_recv.at[source, g], tensor=source,
            ).wait_recv()
    for copy in started:
        copy.wait_send()


def write_out(*refs):
    count = len(refs) // 2
    sems = refs[-1]
    copies = [
        pltpu.make_async_copy(refs[i], refs[count + i], sems.at[i]) for i in range(count)
    ]
    for copy in copies:
        copy.start()
    for copy in copies:
        copy.wait()


def fused_per_device(groups, ranks, hidden_in, value_weight, queries, key_rows, attention_out,
                     output_grad, log_normalizer, document_ids):
    _, tokens, width = hidden_in.shape
    half = value_weight.shape[1]
    hd = 2 * half
    heads = log_normalizer.shape[2]
    span = width // ranks
    sub = span // groups
    chips = groups // 2
    wg_cols = width // groups
    vmem = pl.BlockSpec(memory_space=pltpu.VMEM)
    hbm = pl.BlockSpec(memory_space=pltpu.HBM)
    sem = pltpu.SemaphoreType.DMA
    query_grad, key_grad, input_grad, weight_grad = pl.pallas_call(
        functools.partial(fused, groups, ranks),
        out_shape=(
            jax.ShapeDtypeStruct((tokens, heads * hd), BF16),
            jax.ShapeDtypeStruct((half, tokens), BF16),
            jax.ShapeDtypeStruct((tokens // ranks, width), BF16),
            jax.ShapeDtypeStruct((half, wg_cols), F32),
        ),
        in_specs=[hbm] * 8,
        out_specs=(vmem,) * 4,
        scratch_shapes=[
            pltpu.VMEM((tokens, width), BF16),
            pltpu.VMEM((half, width), BF16),
            pltpu.VMEM((tokens, heads * hd), BF16),
            pltpu.VMEM((tokens, heads * hd), BF16),
            pltpu.VMEM((tokens, heads * hd), BF16),
            pltpu.VMEM((heads, tokens), F32),
            pltpu.VMEM((1, tokens), jnp.int32),
            pltpu.VMEM((ranks * half, span), BF16),
            pltpu.VMEM((2, half, tokens), BF16),
            pltpu.VMEM((2, half, tokens), BF16),
            pltpu.VMEM((heads, tokens, tokens), F32),
            pltpu.VMEM((2, hd, tokens), F32),
            pltpu.VMEM((2, half, tokens), F32),
            pltpu.VMEM((ranks * half, tokens), BF16),
            pltpu.VMEM((groups, tokens, sub), BF16),
            pltpu.VMEM((chips, half, wg_cols), BF16),
            pltpu.VMEM((chips, half, wg_cols), BF16),
            pltpu.VMEM((chips - 1, half, wg_cols), BF16),
            pltpu.VMEM((chips - 1, half, wg_cols), BF16),
            sem((9,)),
            sem((4,)),
            sem((4,)),
            sem((ranks,)),
            sem((ranks,)),
            sem((ranks, groups)),
            sem((ranks, groups)),
            sem((ranks, groups)),
            sem((ranks,)),
            sem((ranks,)),
            sem((chips,)),
            sem((chips,)),
            sem((chips,)),
            sem((chips,)),
            sem((ranks, groups)),
            sem((ranks, groups)),
        ],
        compiler_params=pltpu.CompilerParams(
            collective_id=0, has_side_effects=True, vmem_limit_bytes=56 * 1024 * 1024
        ),
    )(
        hidden_in[0],
        value_weight.T,
        queries[0],
        key_rows[0].T,
        attention_out[0],
        output_grad[0],
        log_normalizer[0].T,
        document_ids,
    )
    results = (query_grad, key_grad, input_grad, weight_grad)
    query_grad, key_grad, input_grad, weight_grad = pl.pallas_call(
        write_out,
        out_shape=tuple(jax.ShapeDtypeStruct(x.shape, x.dtype) for x in results),
        in_specs=[vmem] * len(results),
        out_specs=(hbm,) * len(results),
        scratch_shapes=[sem((len(results),))],
    )(*results)
    return query_grad[None], key_grad.T[None], input_grad[None], weight_grad.T


def partner(value, axis, distance):
    mask = 2**distance
    pairs = [(source, source ^ mask) for source in range(lax.axis_size(axis))]
    return lax.ppermute(value, axis, pairs)


def per_device(
    hidden_in,
    value_weight,
    queries,
    key_rows,
    attention_out,
    output_grad,
    log_normalizer,
    document_ids,
):
    tokens = hidden_in.shape[1]
    head_count = log_normalizer.shape[2]
    half_width = key_rows.shape[2]
    head_width = 2 * half_width
    score_scale = 1.0 / math.sqrt(head_width)
    inputs_local = hidden_in[0]
    value_half = jnp.dot(inputs_local, value_weight, preferred_element_type=jnp.float32).astype(
        jnp.bfloat16
    )
    key_half = key_rows[0]
    other_key, other_value = partner((key_half, value_half), "tensor", 0)
    pair_member = lax.axis_index("tensor") % 2
    lower_member = pair_member == 0
    keys_full = jnp.where(
        lower_member,
        jnp.concatenate([key_half, other_key], 1),
        jnp.concatenate([other_key, key_half], 1),
    )
    values_full = jnp.where(
        lower_member,
        jnp.concatenate([value_half, other_value], 1),
        jnp.concatenate([other_value, value_half], 1),
    )
    query_heads = queries[0].reshape(tokens, head_count, head_width)
    grad_heads = output_grad[0].reshape(tokens, head_count, head_width)
    out_heads = attention_out[0].reshape(tokens, head_count, head_width)
    position = jnp.arange(tokens, dtype=jnp.int32)
    documents = document_ids[0]
    allowed = (position[None, :] <= position[:, None]) & (documents[:, None] == documents[None, :])
    scores = (
        jnp.einsum("thd,sd->hts", query_heads, keys_full, preferred_element_type=jnp.float32)
        * score_scale
    )
    normalizers = jnp.transpose(log_normalizer[0])[:, :, None]
    probabilities = jnp.where(allowed[None], jnp.exp(scores - normalizers), 0.0)
    probs_low = probabilities.astype(jnp.bfloat16)
    value_part = jnp.einsum(
        "hts,thd->sd", probs_low, grad_heads, preferred_element_type=jnp.float32
    )
    row_dots = jnp.einsum("thd,thd->ht", grad_heads, out_heads, preferred_element_type=jnp.float32)
    prob_grad = jnp.einsum(
        "thd,sd->hts", grad_heads, values_full, preferred_element_type=jnp.float32
    )
    score_grad = (probabilities * (prob_grad - row_dots[:, :, None]) * score_scale).astype(
        jnp.bfloat16
    )
    query_grad = jnp.einsum(
        "hts,sd->thd", score_grad, keys_full, preferred_element_type=jnp.float32
    )
    query_grad = query_grad.astype(jnp.bfloat16).reshape(1, tokens, head_count * head_width)
    key_part = jnp.einsum(
        "hts,thd->sd", score_grad, query_heads, preferred_element_type=jnp.float32
    )
    own_offset = pair_member * half_width
    other_offset = (1 - pair_member) * half_width
    send_key = lax.dynamic_slice_in_dim(key_part, other_offset, half_width, 1)
    send_value = lax.dynamic_slice_in_dim(value_part, other_offset, half_width, 1)
    got_key, got_value = partner((send_key, send_value), "tensor", 0)
    key_sum = lax.dynamic_slice_in_dim(key_part, own_offset, half_width, 1) + got_key
    value_sum = lax.dynamic_slice_in_dim(value_part, own_offset, half_width, 1) + got_value
    key_grad = key_sum.astype(jnp.bfloat16).reshape(1, tokens, half_width)
    value_grad = value_sum.astype(jnp.bfloat16)
    input_sum = lax.psum_scatter(
        lax.dot_general(
            value_grad, value_weight, (((1,), (1,)), ((), ())), preferred_element_type=jnp.float32
        ).astype(jnp.bfloat16),
        "tensor",
        scatter_dimension=0,
        tiled=True,
    ).astype(jnp.float32)
    weight_grad = lax.psum_scatter(
        lax.dot_general(
            inputs_local, value_grad, (((0,), (0,)), ((), ())), preferred_element_type=jnp.float32
        ),
        "dp",
        scatter_dimension=0,
        tiled=True,
    )
    input_grad = input_sum.astype(jnp.bfloat16).reshape((1,) + input_sum.shape)
    return (query_grad, key_grad, input_grad, weight_grad)


def solution(mesh):
    groups, ranks = mesh.shape["dp"], mesh.shape["tensor"]

    def body(*operands):
        width = operands[0].shape[2]
        if width % (groups * ranks * 128) == 0:
            return fused_per_device(groups, ranks, *operands)
        return per_device(*operands)

    return jax.shard_map(
        body,
        mesh=mesh,
        in_specs=(
            P("dp", None, None),
            P(None, "tensor"),
            P("dp", None, "tensor"),
            P("dp", None, "tensor"),
            P("dp", None, "tensor"),
            P("dp", None, "tensor"),
            P("dp", None, "tensor"),
            P("dp", None),
        ),
        out_specs=(
            P("dp", None, "tensor"),
            P("dp", None, "tensor"),
            P("dp", "tensor", None),
            P("dp", "tensor"),
        ),
        check_vma=False,
    )
```
